512 devices in a mesh: dp: 64 (over y, z), tensor: 8 (over x, core).
Axes of the slice: x: 4, y: 8, z: 8, core: 2. Of those that a mesh axis runs over, the one named last changes fastest.
Arguments:
- streams: bfloat16 [8192, 4, 8192], P('dp', None, 'tensor'), may hold values from -6 to 6
- layer_out: bfloat16 [8192, 8192], P('dp', 'tensor'), may hold values from -6 to 6
- cotangent: bfloat16 [8192, 4, 8192], P('dp', None, 'tensor'), may hold values from -6 to 6
- input_cot: bfloat16 [8192, 8192], P('dp', 'tensor'), may hold values from -6 to 6
- gain: float32 [8192], P('tensor'), may hold values from 0.5 to 1.5
- projection: float32 [6, 8192], P(None, 'tensor'), may hold values from -0.0625 to 0.0625
- static_mix: float32 [4, 6], replicated, may hold values from -3 to 3
- tanh_scale: float32 [3], replicated, may hold values from 0.5 to 2
Outputs:
- stream_grad: bfloat16 [8192, 4, 8192], P('dp', None, 'tensor')
- out_grad: bfloat16 [8192, 8192], P('dp', 'tensor')
- proj_grad: float32 [6, 8192], P(None, 'tensor')
- gain_grad: float32 [8192], P('tensor')
The draws below stay inside these ranges and needn't reach their ends.
All inputs are finite; a program needn't handle non-finite values.
Results may differ from the reference program's by a relative error of at most 0.0018.
Values sent between devices are 32-bit elements; how exact they have to be, the bound alone decides.
A program may use at most 64 MiB of HBM per device.

```python
import math
import jax
import jax.numpy as jnp
from jax import lax

D = 8192
STREAMS = 4
TOKENS = 8192


def steps_of(own_key, extent, shards, least, largest):
    def one(position, blocks):
        draws = jax.random.uniform(jax.random.fold_in(jax.random.fold_in(own_key, 6), position), (blocks,), jnp.float32, least / len(shards), largest / len(shards))
        return jnp.repeat(jnp.exp(draws), extent[position] // blocks).reshape((-1,) + (1,) * (len(extent) - position - 1))

    factor_of = one(*shards[0])
    for cut in shards[1:]:
        factor_of = factor_of * one(*cut)
    return factor_of


def centred(key, extent, spread, most, cuts=(), held_as=jnp.bfloat16):
    drawn = jax.random.normal(key, extent, jnp.float32) * spread
    if len(cuts) > 0:
        drawn = steps_of(key, extent, cuts, -0.22, 0.18) * drawn
    return jnp.clip(drawn, min=-most, max=most).astype(held_as)


def setup_inputs(seed: int = 0) -> dict:
    arg_keys = jax.random.split(jax.random.key(seed), 9)
    return {
        "streams": centred(arg_keys[0], (TOKENS, STREAMS, D), 1.0, 6.0, ((0, 64), (2, 8))),
        "layer_out": centred(arg_keys[1], (TOKENS, D), 1.0, 6.0, ((0, 64), (1, 8))),
        "cotangent": centred(arg_keys[2], (TOKENS, STREAMS, D), 1.0, 6.0, ((0, 64), (2, 8))),
        "input_cot": centred(arg_keys[3], (TOKENS, D), 1.0, 6.0, ((0, 64), (1, 8))),
        "gain": jnp.clip(1.0 + 0.1 * jax.random.normal(arg_keys[4], (D,), jnp.float32), 0.5, 1.5),
        "projection": centred(arg_keys[5], (6, D), D ** -0.5, 0.0625, ((1, 8),), jnp.float32),
        "static_mix": centred(arg_keys[6], (STREAMS, 6), 0.5, 3.0, (), jnp.float32),
        "tanh_scale": jnp.clip(jnp.exp(jax.random.uniform(arg_keys[7], (3,), jnp.float32, math.log(0.5), math.log(2.0))), 0.5, 2.0),
    }


def reference(streams, layer_out, cotangent, input_cot, gain, projection, static_mix, tanh_scale):
    hidden = streams.astype(jnp.float32)
    grads = cotangent.astype(jnp.float32)
    output = layer_out.astype(jnp.float32)
    back_in = input_cot.astype(jnp.float32)
    wproj = gain[None, :] * projection
    square = jnp.einsum('tjd,tjd->tj', hidden, hidden, precision=lax.Precision.HIGHEST)
    lin = jnp.einsum('tjd,cd->tjc', hidden, wproj, precision=lax.Precision.HIGHEST)
    dbeta = jnp.einsum('td,tkd->tk', output, grads, precision=lax.Precision.HIGHEST)
    dalpha = jnp.einsum('tjd,td->tj', hidden, back_in, precision=lax.Precision.HIGHEST)
    dmixer = jnp.einsum('tjd,tkd->tjk', hidden, grads, precision=lax.Precision.HIGHEST)
    inv_rms = lax.rsqrt(square / D + 1e-06)
    bent = jnp.tanh(inv_rms[..., None] * lin)
    scales = jnp.concatenate([tanh_scale[0:2], jnp.repeat(tanh_scale[2:3], 4)])
    coef = static_mix[None] + scales * bent
    dcoef = jnp.concatenate([dbeta[..., None], dalpha[..., None], dmixer], axis=-1)
    dpre = dcoef * scales * (1.0 - bent * bent)
    dlin = dpre * inv_rms[..., None]
    dsquare = -0.5 * inv_rms ** 3 / D * lax.optimization_barrier(jnp.sum(dpre * lin, axis=-1))
    out_grad = jnp.einsum('tk,tkd->td', coef[:, :, 0], grads, precision=lax.Precision.HIGHEST).astype(jnp.bfloat16)
    total = jnp.einsum('tjk,tkd->tjd', coef[:, :, 2:], grads, precision=lax.Precision.HIGHEST)
    total = total + coef[:, :, 1][..., None] * back_in[:, None, :]
    total = total + jnp.einsum('tjc,cd->tjd', dlin, wproj, precision=lax.Precision.HIGHEST)
    total = total + 2.0 * dsquare[..., None] * hidden
    stream_grad = total.astype(jnp.bfloat16)
    dweight = jnp.einsum('tjc,tjd->cd', dlin, hidden, precision=lax.Precision.HIGHEST)
    proj_grad = gain[None, :] * dweight / jnp.sqrt(4.0 * TOKENS * D)
    gain_grad = lax.optimization_barrier(jnp.sum(dweight * projection, axis=0)) / jnp.sqrt(4.0 * TOKENS)
    return (stream_grad, out_grad, proj_grad, gain_grad)
```

```python
import functools

import jax
import jax.numpy as jnp
from jax import lax
from jax.experimental import pallas as pl
from jax.experimental.pallas import tpu as pltpu
from jax.sharding import PartitionSpec as P

D = 8192
F32, BF16 = jnp.float32, jnp.bfloat16
NT = (((1,), (1,)), ((), ()))
NN = (((1,), (0,)), ((), ()))
TN = (((0,), (0,)), ((), ()))
GROUPS = 4
SPAN = 32
FAR_X = ((2, 0), (2, 1), (1, 0), (3, 0), (1, 1), (3, 1), (0, 1))
FAR = (4, 3, 5, 2, 6, 1, 7)
ROWS = 320


def mm(a, b, dims):
    return lax.dot_general(a, b, dims, preferred_element_type=F32)


def split(v):
    high = v.astype(BF16).astype(F32)
    return high, v - high


def body(
    h_hbm, y_hbm, g_hbm, g0_hbm, gain_hbm, proj_hbm, mix_hbm, ts_hbm,
    sg_hbm, og_hbm, pg_out, gg_out,
    h_raw, g_raw, y_s, x_s, gain_s, proj_s, mix_s, ts_s, w_s, stat, dw1, dw2, got1, got2, sg_s, og_s,
    load_sem, small_sem, out_sem, st_send, st_recv, dw_send, dw_recv,
):
    dp, tensor = lax.axis_index("dp"), lax.axis_index("tensor")
    x, core = tensor // 2, tensor % 2
    yy, zz = dp // 8, dp % 8

    smalls = [
        pltpu.make_async_copy(src, dst, small_sem.at[n])
        for n, (src, dst) in enumerate(((gain_hbm, gain_s), (proj_hbm, proj_s), (mix_hbm, mix_s), (ts_hbm, ts_s)))
    ]
    loads = []
    for i in range(GROUPS):
        part = pl.ds(i * SPAN, SPAN)
        loads.append([
            pltpu.make_async_copy(h_hbm.at[part], h_raw.at[part], load_sem.at[i, 0]),
            pltpu.make_async_copy(g_hbm.at[part], g_raw.at[part], load_sem.at[i, 1]),
            pltpu.make_async_copy(g0_hbm.at[part], x_s.at[i, pl.ds(256, SPAN)], load_sem.at[i, 2]),
            pltpu.make_async_copy(y_hbm.at[part], y_s.at[part], load_sem.at[i, 3]),
        ])
    for copy in loads[0] + smalls + loads[1] + loads[2] + loads[3]:
        copy.start()

    def tensor_peer(dx, dc):
        return {"dp": dp, "tensor": ((x + dx) % 4) * 2 + (core + dc) % 2}

    def y_peer(dy):
        return {"dp": ((yy + dy) % 8) * 8 + zz, "tensor": tensor}

    def z_peer(dz):
        return {"dp": yy * 8 + (zz + dz) % 8, "tensor": tensor}

    barrier = pltpu.get_barrier_semaphore()
    peers = [tensor_peer(*d) for d in FAR_X] + [y_peer(d) for d in FAR] + [z_peer(d) for d in FAR]
    for peer in peers:
        pl.semaphore_signal(barrier, inc=1, device_id=peer, device_id_type=pl.DeviceIdType.MESH)

    row8 = lax.broadcasted_iota(jnp.int32, (8, 128), 0)
    lane8 = lax.broadcasted_iota(jnp.int32, (8, 128), 1)
    row = lax.broadcasted_iota(jnp.int32, (128, 128), 0)
    lane = lax.broadcasted_iota(jnp.int32, (128, 128), 1)
    same = row == lane
    token = (row // 4) == (lane // 4)
    owner = row[:SPAN] == (lane[:SPAN] // 4)

    for copy in smalls:
        copy.wait()
    w_s[...] = jnp.zeros_like(w_s)
    w_s[0:6, :] = gain_s[...] * proj_s[...]
    w_hi, w_rest = split(w_s[...])
    w_mid, w_lo = split(w_rest)
    w_all = jnp.concatenate([w_hi, w_mid, w_lo, jnp.zeros_like(w_lo)], axis=0).astype(BF16)
    for i in range(GROUPS):
        x_s[i, 288:320, :] = w_all
    mixv = jnp.zeros((8, 128), F32)
    for c in range(6):
        for j in range(4):
            mixv = jnp.where((row8 == c) & (lane8 % 4 == j), mix_s[j, c], mixv)
    sv = jnp.where(row8 == 0, ts_s[0], jnp.where(row8 == 1, ts_s[1], jnp.where(row8 < 6, ts_s[2], 0.0)))

    def send_stats(i):
        copies = []
        for n, (dx, dc) in enumerate(FAR_X):
            copies.append(
                pltpu.make_async_remote_copy(
                    src_ref=stat.at[tensor, i], dst_ref=stat.at[tensor, i],
                    send_sem=st_send.at[i, n], recv_sem=st_recv.at[i, tensor],
                    device_id=tensor_peer(dx, dc), device_id_type=pl.DeviceIdType.MESH,
                )
            )
        for copy in copies:
            copy.start()
        return copies

    sends = []
    for i in range(GROUPS):
        for copy in loads[i]:
            copy.wait()
        part = pl.ds(i * SPAN, SPAN)
        x_s[i, 0:128, :] = h_raw[part].reshape(128, 1024)
        x_s[i, 128:256, :] = g_raw[part].reshape(128, 1024)
        p1 = mm(x_s[i], x_s[i, 0:128, :], NT)
        p2 = mm(y_s[part, :], x_s[i, 128:256, :], NT)
        square = jnp.sum(jnp.where(same, p1[0:128], 0.0), axis=0, keepdims=True)
        dmix = jnp.sum(jnp.where(token, p1[128:256], 0.0).reshape(16, 8, 128), axis=0)
        dmix = dmix + pltpu.roll(dmix, 4, 0)
        dalpha = jnp.sum(jnp.where(owner, p1[256:288], 0.0), axis=0, keepdims=True)
        dbeta = jnp.sum(jnp.where(owner, p2, 0.0), axis=0, keepdims=True)
        lin = p1[288:296] + p1[296:304] + p1[304:312]
        stat[tensor, i, 0:8, :] = jnp.where(row8 == 6, square, lin)
        stat[tensor, i, 8:16, :] = jnp.where(
            row8 == 0, dbeta, jnp.where(row8 == 1, dalpha, jnp.where(row8 < 6, pltpu.roll(dmix, 2, 0), 0.0))
        )
        if i == 0:
            pl.semaphore_wait(barrier, len(peers))
        sends += send_stats(i)

    coefs, dlins, dsq2s = [], [], []
    dw = jnp.zeros((8, 1024), F32)
    for i in range(GROUPS):
        for dx, dc in FAR_X:
            other = ((x + dx) % 4) * 2 + (core + dc) % 2
            pltpu.make_async_remote_copy(
                src_ref=stat.at[other, i], dst_ref=stat.at[other, i],
                send_sem=st_send.at[i, 0], recv_sem=st_recv.at[i, other],
                device_id=tensor_peer(dx, dc), device_id_type=pl.DeviceIdType.MESH,
            ).wait_recv()
        total = stat[0, i]
        for n in range(1, 8):
            total = total + stat[n, i]
        lin, dcoef = total[0:8], total[8:16]
        inv = lax.rsqrt(total[6:7] / D + 1e-06)
        bent = jnp.tanh(inv * lin)
        dpre = dcoef * sv * (1.0 - bent * bent)
        dlin = dpre * inv
        coefs.append(mixv + sv * bent)
        dlins.append(dlin)
        dsq2s.append(-1.0 * (inv * inv * inv) / D * jnp.sum(dpre * lin, axis=0, keepdims=True))
        d_hi, d_rest = split(dlin)
        d_mid, d_lo = split(d_rest)
        left = jnp.concatenate([d_hi, d_mid, d_lo, jnp.zeros_like(d_lo)], axis=0).astype(BF16)
        part = mm(left, x_s[i, 0:128, :], NN)
        dw = dw + (part[0:8] + part[8:16] + part[16:24])

    for q in range(8):
        a, b = q // 4, q % 4
        dw1[a, 6 * b : 6 * b + 6, :] = dw[0:6, 128 * q : 128 * q + 128]

    def exchange(step, source, got, along):
        own = (yy, zz)
        copies = []
        for n, far in enumerate(FAR):
            for a in range(2):
                axis = along[a]
                copies.append(
                    pltpu.make_async_remote_copy(
                        src_ref=source.at[a], dst_ref=got.at[a, own[axis]],
                        send_sem=dw_send.at[step, a, n], recv_sem=dw_recv.at[step, a, own[axis]],
                        device_id=(y_peer, z_peer)[axis](far), device_id_type=pl.DeviceIdType.MESH,
                    )
                )
        for copy in copies:
            copy.start()
        for a in range(2):
            got[a, own[along[a]]] = source[a]
        return copies

    def arrive(step, source, got, along):
        own = (yy, zz)
        for far in FAR:
            for a in range(2):
                other = (own[along[a]] + far) % 8
                pltpu.make_async_remote_copy(
                    src_ref=source.at[a], dst_ref=got.at[a, other],
                    send_sem=dw_send.at[step, a, 0], recv_sem=dw_recv.at[step, a, other],
                    device_id=(y_peer, z_peer)[along[a]](far), device_id_type=pl.DeviceIdType.MESH,
                ).wait_recv()
        sums = []
        for a in range(2):
            total = got[a, 0]
            for n in range(1, 8):
                total = total + got[a, n]
            sums.append(total)
        return sums

    def grads(i):
        coef, dlin, dsq2 = coefs[i], dlins[i], dsq2s[i]
        mix8 = jnp.where(row8 < 4, pltpu.roll(coef, 6, 0), pltpu.roll(coef, 2, 0))
        mixer = jnp.where(token, jnp.broadcast_to(mix8[None], (16, 8, 128)).reshape(128, 128), 0.0)
        diag = jnp.where(same, dsq2, 0.0)
        alpha = jnp.where(owner, coef[1:2], 0.0)
        left = jnp.concatenate([diag, mixer, alpha, dlin, dlin, dlin, jnp.zeros_like(dlin)], axis=0)
        high, low = split(left)
        both = jnp.concatenate([high.T, low.T], axis=0).astype(BF16)
        beta = jnp.where(owner, coef[0:1], 0.0)
        b_high, b_low = split(beta)
        b_both = jnp.concatenate([b_high, b_low], axis=0).astype(BF16)
        part = pl.ds(i * SPAN, SPAN)
        for n in range(4):
            columns = slice(256 * n, 256 * n + 256)
            out = mm(both, x_s[i, :, columns], NN)
            sg_s[part, :, columns] = (out[0:128] + out[128:256]).astype(BF16).reshape(SPAN, 4, 256)
            out = mm(b_both, x_s[i, 128:256, columns], NN)
            og_s[part, columns] = (out[0:SPAN] + out[SPAN : 2 * SPAN]).astype(BF16)
        copies = [
            pltpu.make_async_copy(sg_s.at[part], sg_hbm.at[part], out_sem.at[i, 0]),
            pltpu.make_async_copy(og_s.at[part], og_hbm.at[part], out_sem.at[i, 1]),
        ]
        for copy in copies:
            copy.start()
        return copies

    sends += exchange(0, dw1, got1, (0, 1))
    stores = grads(0) + grads(1)
    for a, total in enumerate(arrive(0, dw1, got1, (0, 1))):
        dw2[a] = total
    sends += exchange(1, dw2, got2, (1, 0))
    stores += grads(2) + grads(3)
    sums = arrive(1, dw2, got2, (1, 0))
    per_proj = 1.0 / (4.0 * 64 * 128 * D) ** 0.5
    per_gain = 1.0 / (4.0 * 64 * 128) ** 0.5
    for q in range(8):
        a, b = q // 4, q % 4
        columns = slice(128 * q, 128 * q + 128)
        total = sums[a][6 * b : 6 * b + 6]
        pg_out[:, columns] = gain_s[:, columns] * total * per_proj
        gg_out[:, columns] = jnp.sum(total * proj_s[:, columns], axis=0, keepdims=True) * per_gain
    for copy in stores:
        copy.wait()
    for copy in sends:
        copy.wait_send()


def shards(streams, layer_out, cotangent, input_cot, gain, projection, static_mix, tanh_scale):
    anywhere = pl.BlockSpec(memory_space=pl.ANY)
    vmem = pl.BlockSpec(memory_space=pltpu.VMEM)
    sg, og, pg, gg = pl.pallas_call(
        body,
        out_shape=(
            jax.ShapeDtypeStruct(streams.shape, BF16),
            jax.ShapeDtypeStruct(layer_out.shape, BF16),
            jax.ShapeDtypeStruct((6, 1024), F32),
            jax.ShapeDtypeStruct((1, 1024), F32),
        ),
        in_specs=[anywhere] * 8,
        out_specs=(anywhere, anywhere, vmem, vmem),
        scratch_shapes=[
            pltpu.VMEM((128, 4, 1024), BF16),
            pltpu.VMEM((128, 4, 1024), BF16),
            pltpu.VMEM((128, 1024), BF16),
            pltpu.VMEM((GROUPS, ROWS, 1024), BF16),
            pltpu.VMEM((1, 1024), F32),
            pltpu.VMEM((6, 1024), F32),
            pltpu.SMEM((4, 6), F32),
            pltpu.SMEM((3,), F32),
            pltpu.VMEM((8, 1024), F32),
            pltpu.VMEM((8, GROUPS, 16, 128), F32),
            pltpu.VMEM((2, 24, 128), F32),
            pltpu.VMEM((2, 24, 128), F32),
            pltpu.VMEM((2, 8, 24, 128), F32),
            pltpu.VMEM((2, 8, 24, 128), F32),
            pltpu.VMEM((128, 4, 1024), BF16),
            pltpu.VMEM((128, 1024), BF16),
            pltpu.SemaphoreType.DMA((GROUPS, 4)),
            pltpu.SemaphoreType.DMA((4,)),
            pltpu.SemaphoreType.DMA((GROUPS, 2)),
            pltpu.SemaphoreType.DMA((GROUPS, 7)),
            pltpu.SemaphoreType.DMA((GROUPS, 8)),
            pltpu.SemaphoreType.DMA((2, 2, 7)),
            pltpu.SemaphoreType.DMA((2, 2, 8)),
        ],
        compiler_params=pltpu.CompilerParams(collective_id=0, has_side_effects=True),
    )(streams, layer_out, cotangent, input_cot, gain.reshape(1, 1024), projection, static_mix, tanh_scale)
    return sg, og, pg, gg.reshape(1024)


def solution(mesh):
    placed = (
        P("dp", None, "tensor"),
        P("dp", "tensor"),
        P("dp", None, "tensor"),
        P("dp", "tensor"),
        P("tensor"),
        P(None, "tensor"),
        P(),
        P(),
    )
    return jax.shard_map(
        shards,
        mesh=mesh,
        in_specs=placed,
        out_specs=(P("dp", None, "tensor"), P("dp", "tensor"), P(None, "tensor"), P("tensor")),
        check_vma=False,
    )
```

```python
import functools

import jax
import jax.numpy as jnp
from jax import lax
from jax.experimental import pallas as pl
from jax.experimental.pallas import tpu as pltpu
from jax.sharding import PartitionSpec as P

D = 8192
F32, BF16 = jnp.float32, jnp.bfloat16
NT = (((1,), (1,)), ((), ()))
NN = (((1,), (0,)), ((), ()))
TN = (((0,), (0,)), ((), ()))
GROUPS = 4
SPAN = 32
FAR_X = ((2, 0), (2, 1), (1, 0), (3, 0), (1, 1), (3, 1), (0, 1))
FAR = (4, 3, 5, 2, 6, 1, 7)
ROWS = 320


def mm(a, b, dims):
    return lax.dot_general(a, b, dims, preferred_element_type=F32)


def split(v):
    high = v.astype(BF16).astype(F32)
    return high, v - high


def body(
    h_hbm, y_hbm, g_hbm, g0_hbm, gain_hbm, proj_hbm, mix_hbm, ts_hbm,
    sg_s, og_s, pg_out, gg_out,
    h_raw, g_raw, y_s, x_s, gain_s, proj_s, mix_s, ts_s, w_s, own_s, near_s, stat, dw1, dw2, got1, got2,
    load_sem, small_sem, near_send, near_recv, st_send, st_recv, dw_send, dw_recv,
):
    dp, tensor = lax.axis_index("dp"), lax.axis_index("tensor")
    x, core = tensor // 2, tensor % 2
    yy, zz = dp // 8, dp % 8

    smalls = [
        pltpu.make_async_copy(src, dst, small_sem.at[n])
        for n, (src, dst) in enumerate(((gain_hbm, gain_s), (proj_hbm, proj_s), (mix_hbm, mix_s), (ts_hbm, ts_s)))
    ]
    loads = []
    order = (1 - core, 3 - core, core, 2 + core)
    for k, g in enumerate(order):
        part = pl.ds(pl.multiple_of(g * SPAN, SPAN), SPAN)
        loads.append([
            pltpu.make_async_copy(h_hbm.at[part], h_raw.at[part], load_sem.at[k, 0]),
            pltpu.make_async_copy(g_hbm.at[part], g_raw.at[part], load_sem.at[k, 1]),
            pltpu.make_async_copy(g0_hbm.at[part], x_s.at[g, pl.ds(256, SPAN)], load_sem.at[k, 2]),
            pltpu.make_async_copy(y_hbm.at[part], y_s.at[g], load_sem.at[k, 3]),
        ])
    for copy in loads[0] + smalls + loads[1] + loads[2] + loads[3]:
        copy.start()

    def tensor_peer(dx, dc):
        return {"dp": dp, "tensor": ((x + dx) % 4) * 2 + (core + dc) % 2}

    def y_peer(dy):
        return {"dp": ((yy + dy) % 8) * 8 + zz, "tensor": tensor}

    def z_peer(dz):
        return {"dp": yy * 8 + (zz + dz) % 8, "tensor": tensor}

    barrier = pltpu.get_barrier_semaphore()
    peers = [tensor_peer(*d) for d in FAR_X] + [y_peer(d) for d in FAR] + [z_peer(d) for d in FAR]
    for peer in peers:
        pl.semaphore_signal(barrier, inc=1, device_id=peer, device_id_type=pl.DeviceIdType.MESH)

    row8 = lax.broadcasted_iota(jnp.int32, (8, 128), 0)
    lane8 = lax.broadcasted_iota(jnp.int32, (8, 128), 1)
    row = lax.broadcasted_iota(jnp.int32, (128, 128), 0)
    lane = lax.broadcasted_iota(jnp.int32, (128, 128), 1)
    same = row == lane
    token = (row // 4) == (lane // 4)
    owner = row[:SPAN] == (lane[:SPAN] // 4)

    for copy in smalls:
        copy.wait()
    w_s[...] = jnp.zeros_like(w_s)
    w_s[0:6, :] = gain_s[...] * proj_s[...]
    w_hi, w_rest = split(w_s[...])
    w_mid, w_lo = split(w_rest)
    w_all = jnp.concatenate([w_hi, w_mid, w_lo, jnp.zeros_like(w_lo)], axis=0).astype(BF16)
    for i in range(GROUPS):
        x_s[i, 288:320, :] = w_all
    mixv = jnp.zeros((8, 128), F32)
    for c in range(6):
        for j in range(4):
            mixv = jnp.where((row8 == c) & (lane8 % 4 == j), mix_s[j, c], mixv)
    sv = jnp.where(row8 == 0, ts_s[0], jnp.where(row8 == 1, ts_s[1], jnp.where(row8 < 6, ts_s[2], 0.0)))

    def inner(g, k):
        for copy in loads[k]:
            copy.wait()
        x_s[g, 0:128, :] = h_raw[pl.ds(g * SPAN, SPAN)].reshape(128, 1024)
        x_s[g, 128:256, :] = g_raw[pl.ds(g * SPAN, SPAN)].reshape(128, 1024)
        p1 = mm(x_s[g], x_s[g, 0:128, :], NT)
        p2 = mm(y_s[g], x_s[g, 128:256, :], NT)
        square = jnp.sum(jnp.where(same, p1[0:128], 0.0), axis=0, keepdims=True)
        dmix = jnp.sum(jnp.where(token, p1[128:256], 0.0).reshape(16, 8, 128), axis=0)
        dmix = dmix + pltpu.roll(dmix, 4, 0)
        dalpha = jnp.sum(jnp.where(owner, p1[256:288], 0.0), axis=0, keepdims=True)
        dbeta = jnp.sum(jnp.where(owner, p2, 0.0), axis=0, keepdims=True)
        lin = p1[288:296] + p1[296:304] + p1[304:312]
        own_s[g, 0:8, :] = jnp.where(row8 == 6, square, lin)
        own_s[g, 8:16, :] = jnp.where(
            row8 == 0, dbeta, jnp.where(row8 == 1, dalpha, jnp.where(row8 < 6, pltpu.roll(dmix, 2, 0), 0.0))
        )

    def pass_on(k):
        g = order[k]
        return pltpu.make_async_remote_copy(
            src_ref=own_s.at[g], dst_ref=near_s.at[k],
            send_sem=near_send.at[k], recv_sem=near_recv.at[k],
            device_id=tensor_peer(0, 1), device_id_type=pl.DeviceIdType.MESH,
        )

    sends = []
    for k in range(GROUPS):
        inner(order[k], k)
        if k == 0:
            pl.semaphore_wait(barrier, len(peers))
        if k < 2:
            copy = pass_on(k)
            copy.start()
            sends.append(copy)
    for k in range(2):
        g = order[2 + k]
        pass_on(k).wait_recv()
        stat[x, g] = own_s[g] + near_s[k]
        copies = [
            pltpu.make_async_remote_copy(
                src_ref=stat.at[x, g], dst_ref=stat.at[x, g],
                send_sem=st_send.at[k, n], recv_sem=st_recv.at[x, g],
                device_id=tensor_peer(dx, dc), device_id_type=pl.DeviceIdType.MESH,
            )
            for n, (dx, dc) in enumerate(FAR_X)
        ]
        for copy in copies:
            copy.start()
        sends += copies

    def stats_in(chip, g):
        pltpu.make_async_remote_copy(
            src_ref=stat.at[chip, g], dst_ref=stat.at[chip, g],
            send_sem=st_send.at[0, 0], recv_sem=st_recv.at[chip, g],
            device_id=tensor_peer(0, 1), device_id_type=pl.DeviceIdType.MESH,
        ).wait_recv()

    coefs, dlins, dsq2s = [], [], []
    dw = jnp.zeros((8, 1024), F32)
    for k in range(2):
        stats_in(x, order[k])
        for dx in (1, 3, 2):
            for n in range(2):
                stats_in((x + dx) % 4, 2 * k + n)
        for i in (2 * k, 2 * k + 1):
            total = (stat[0, i] + stat[1, i]) + (stat[2, i] + stat[3, i])
            lin, dcoef = total[0:8], total[8:16]
            inv = lax.rsqrt(total[6:7] / D + 1e-06)
            bent = jnp.tanh(inv * lin)
            dpre = dcoef * sv * (1.0 - bent * bent)
            dlin = dpre * inv
            coefs.append(mixv + sv * bent)
            dlins.append(dlin)
            dsq2s.append(-1.0 * (inv * inv * inv) / D * jnp.sum(dpre * lin, axis=0, keepdims=True))
            d_hi, d_lo = split(dlin)
            left = jnp.concatenate([d_hi, d_lo], axis=0).astype(BF16)
            part = mm(left, x_s[i, 0:128, :], NN)
            dw = dw + (part[0:8] + part[8:16])

    for q in range(8):
        a, b = q // 4, q % 4
        dw1[a, 6 * b : 6 * b + 6, :] = dw[0:6, 128 * q : 128 * q + 128]

    def exchange(step, source, got, along):
        own = (yy, zz)
        copies = []
        for n, far in enumerate(FAR):
            for a in range(2):
                axis = along[a]
                copies.append(
                    pltpu.make_async_remote_copy(
                        src_ref=source.at[a], dst_ref=got.at[a, own[axis]],
                        send_sem=dw_send.at[step, a, n], recv_sem=dw_recv.at[step, a, own[axis]],
                        device_id=(y_peer, z_peer)[axis](far), device_id_type=pl.DeviceIdType.MESH,
                    )
                )
        for copy in copies:
            copy.start()
        for a in range(2):
            got[a, own[along[a]]] = source[a]
        return copies

    def arrive(step, source, got, along):
        own = (yy, zz)
        for far in FAR:
            for a in range(2):
                other = (own[along[a]] + far) % 8
                pltpu.make_async_remote_copy(
                    src_ref=source.at[a], dst_ref=got.at[a, other],
                    send_sem=dw_send.at[step, a, 0], recv_sem=dw_recv.at[step, a, other],
                    device_id=(y_peer, z_peer)[along[a]](far), device_id_type=pl.DeviceIdType.MESH,
                ).wait_recv()
        sums = []
        for a in range(2):
            total = got[a, 0]
            for n in range(1, 8):
                total = total + got[a, n]
            sums.append(total)
        return sums

    def grads(i):
        coef, dlin, dsq2 = coefs[i], dlins[i], dsq2s[i]
        mix8 = jnp.where(row8 < 4, pltpu.roll(coef, 6, 0), pltpu.roll(coef, 2, 0))
        mixer = jnp.where(token, jnp.broadcast_to(mix8[None], (16, 8, 128)).reshape(128, 128), 0.0)
        diag = jnp.where(same, dsq2, 0.0)
        alpha = jnp.where(owner, coef[1:2], 0.0)
        left = jnp.concatenate([diag, mixer, alpha, dlin, dlin, dlin, jnp.zeros_like(dlin)], axis=0)
        high, low = split(left)
        both = jnp.concatenate([high.T, low.T], axis=0).astype(BF16)
        beta = jnp.where(owner, coef[0:1], 0.0)
        b_high, b_low = split(beta)
        b_both = jnp.concatenate([b_high, b_low], axis=0).astype(BF16)
        part = pl.ds(i * SPAN, SPAN)
        for n in range(4):
            columns = slice(256 * n, 256 * n + 256)
            out = mm(both, x_s[i, :, columns], NN)
            sg_s[part, :, columns] = (out[0:128] + out[128:256]).astype(BF16).reshape(SPAN, 4, 256)
            out = mm(b_both, x_s[i, 128:256, columns], NN)
            og_s[part, columns] = (out[0:SPAN] + out[SPAN : 2 * SPAN]).astype(BF16)

    sends += exchange(0, dw1, got1, (0, 1))
    grads(0)
    grads(1)
    for a, total in enumerate(arrive(0, dw1, got1, (0, 1))):
        dw2[a] = total
    sends += exchange(1, dw2, got2, (1, 0))
    grads(2)
    grads(3)
    sums = arrive(1, dw2, got2, (1, 0))
    per_proj = 1.0 / (4.0 * 64 * 128 * D) ** 0.5
    per_gain = 1.0 / (4.0 * 64 * 128) ** 0.5
    for q in range(8):
        a, b = q // 4, q % 4
        columns = slice(128 * q, 128 * q + 128)
        total = sums[a][6 * b : 6 * b + 6]
        pg_out[:, columns] = gain_s[:, columns] * total * per_proj
        gg_out[:, columns] = jnp.sum(total * proj_s[:, columns], axis=0, keepdims=True) * per_gain
    for copy in sends:
        copy.wait_send()


def store(*refs):
    copies = [pltpu.make_async_copy(refs[n], refs[4 + n], refs[8].at[n]) for n in range(4)]
    for copy in copies:
        copy.start()
    for copy in copies:
        copy.wait()


def shards(streams, layer_out, cotangent, input_cot, gain, projection, static_mix, tanh_scale):
    anywhere = pl.BlockSpec(memory_space=pl.ANY)
    vmem = pl.BlockSpec(memory_space=pltpu.VMEM)
    sg, og, pg, gg = pl.pallas_call(
        body,
        out_shape=(
            pltpu.VMEM(streams.shape, BF16),
            pltpu.VMEM(layer_out.shape, BF16),
            pltpu.VMEM((6, 1024), F32),
            pltpu.VMEM((1, 1024), F32),
        ),
        in_specs=[anywhere] * 8,
        out_specs=(vmem,) * 4,
        scratch_shapes=[
            pltpu.VMEM((128, 4, 1024), BF16),
            pltpu.VMEM((128, 4, 1024), BF16),
            pltpu.VMEM((GROUPS, SPAN, 1024), BF16),
            pltpu.VMEM((GROUPS, ROWS, 1024), BF16),
            pltpu.VMEM((1, 1024), F32),
            pltpu.VMEM((6, 1024), F32),
            pltpu.SMEM((4, 6), F32),
            pltpu.SMEM((3,), F32),
            pltpu.VMEM((8, 1024), F32),
            pltpu.VMEM((GROUPS, 16, 128), F32),
            pltpu.VMEM((2, 16, 128), F32),
            pltpu.VMEM((4, GROUPS, 16, 128), F32),
            pltpu.VMEM((2, 24, 128), F32),
            pltpu.VMEM((2, 24, 128), F32),
            pltpu.VMEM((2, 8, 24, 128), F32),
            pltpu.VMEM((2, 8, 24, 128), F32),
            pltpu.SemaphoreType.DMA((GROUPS, 4)),
            pltpu.SemaphoreType.DMA((4,)),
            pltpu.SemaphoreType.DMA((2,)),
            pltpu.SemaphoreType.DMA((2,)),
            pltpu.SemaphoreType.DMA((2, 7)),
            pltpu.SemaphoreType.DMA((4, GROUPS)),
            pltpu.SemaphoreType.DMA((2, 2, 7)),
            pltpu.SemaphoreType.DMA((2, 2, 8)),
        ],
        compiler_params=pltpu.CompilerParams(collective_id=0, has_side_effects=True),
    )(streams, layer_out, cotangent, input_cot, gain.reshape(1, 1024), projection, static_mix, tanh_scale)
    made = (sg, og, pg, gg)
    sg, og, pg, gg = pl.pallas_call(
        store,
        out_shape=tuple(jax.ShapeDtypeStruct(a.shape, a.dtype) for a in made),
        in_specs=[vmem] * 4,
        out_specs=(anywhere,) * 4,
        scratch_shapes=[pltpu.SemaphoreType.DMA((4,))],
    )(*(pltpu.with_memory_space_constraint(a, pltpu.VMEM) for a in made))
    return sg, og, pg, gg.reshape(1024)


def solution(mesh):
    placed = (
        P("dp", None, "tensor"),
        P("dp", "tensor"),
        P("dp", None, "tensor"),
        P("dp", "tensor"),
        P("tensor"),
        P(None, "tensor"),
        P(),
        P(),
    )
    return jax.shard_map(
        shards,
        mesh=mesh,
        in_specs=placed,
        out_specs=(P("dp", None, "tensor"), P("dp", "tensor"), P(None, "tensor"), P("tensor")),
        check_vma=False,
    )
```

```python
import functools

import jax
import jax.numpy as jnp
from jax import lax
from jax.experimental import pallas as pl
from jax.experimental.pallas import tpu as pltpu
from jax.sharding import PartitionSpec as P

D = 8192
F32, BF16 = jnp.float32, jnp.bfloat16
NT = (((1,), (1,)), ((), ()))
NN = (((1,), (0,)), ((), ()))
TN = (((0,), (0,)), ((), ()))
GROUPS = 4
SPAN = 32
FAR_X = ((2, 0), (2, 1), (1, 0), (3, 0), (1, 1), (3, 1), (0, 1))
ROWS = 320


def mm(a, b, dims):
    return lax.dot_general(a, b, dims, preferred_element_type=F32)


def split(v):
    high = v.astype(BF16).astype(F32)
    return high, v - high


def body(
    h_hbm, y_hbm, g_hbm, g0_hbm, gain_hbm, proj_hbm, mix_hbm, ts_hbm,
    sg_s, og_s, pg_out, gg_out,
    h_raw, g_raw, y_s, x_s, gain_s, proj_s, mix_s, ts_s, w_s, own_s, near_s, stat, coef_s, dw1, dw2, got1, got2,
    load_sem, small_sem, near_recv, st_send, st_recv, dw_send, dw_recv,
):
    dp, tensor = lax.axis_index("dp"), lax.axis_index("tensor")
    x, core = tensor // 2, tensor % 2
    yy, zz = dp // 8, dp % 8

    order = (1 - core, 3 - core, core, 2 + core)

    def loads(k):
        part = pl.ds(pl.multiple_of(order[k] * SPAN, SPAN), SPAN)
        for src, dst in (
            (h_hbm.at[part], h_raw.at[part]),
            (g_hbm.at[part], g_raw.at[part]),
            (g0_hbm.at[part], x_s.at[order[k], pl.ds(256, SPAN)]),
            (y_hbm.at[part], y_s.at[order[k]]),
        ):
            pltpu.make_async_copy(src, dst, load_sem.at[k]).start()

    smalls = [
        pltpu.make_async_copy(src, dst, small_sem.at[n])
        for n, (src, dst) in enumerate(((mix_hbm, mix_s), (ts_hbm, ts_s), (gain_hbm, gain_s), (proj_hbm, proj_s)))
    ]
    for copy in smalls:
        copy.start()
    loads(0)

    def arrived(like, sem):
        pltpu.make_async_copy(like, like, sem).wait()

    def tensor_peer(dx, dc):
        return {"dp": dp, "tensor": ((x + dx) % 4) * 2 + (core + dc) % 2}

    def y_peer(n):
        return {"dp": (n + (n + 8 - yy) // 8) * 8 + zz, "tensor": tensor}

    def z_peer(n):
        return {"dp": yy * 8 + n + (n + 8 - zz) // 8, "tensor": tensor}

    barrier = pltpu.get_barrier_semaphore()
    peers = [peer(n) for n in range(7) for peer in (y_peer, z_peer)] + [tensor_peer(*d) for d in FAR_X]
    for peer in peers:
        pl.semaphore_signal(barrier, inc=1, device_id=peer, device_id_type=pl.DeviceIdType.MESH)
    for k in range(1, GROUPS):
        loads(k)

    row8 = lax.broadcasted_iota(jnp.int32, (8, 128), 0)
    lane8 = lax.broadcasted_iota(jnp.int32, (8, 128), 1)
    row = lax.broadcasted_iota(jnp.int32, (128, 128), 0)
    lane = lax.broadcasted_iota(jnp.int32, (128, 128), 1)
    same = row == lane
    token = (row // 4) == (lane // 4)
    owner = row[:SPAN] == (lane[:SPAN] // 4)

    for copy in smalls:
        copy.wait()
    w_s[...] = jnp.zeros_like(w_s)
    w_s[0:6, :] = gain_s[...] * proj_s[...]
    w_hi, w_rest = split(w_s[...])
    w_mid, w_lo = split(w_rest)
    w_all = jnp.concatenate([w_hi, w_mid, w_lo, jnp.zeros_like(w_lo)], axis=0).astype(BF16)
    for i in range(GROUPS):
        x_s[i, 288:320, :] = w_all
    mixv = jnp.zeros((8, 128), F32)
    for c in range(6):
        for j in range(4):
            mixv = jnp.where((row8 == c) & (lane8 % 4 == j), mix_s[j, c], mixv)
    sv = jnp.where(row8 == 0, ts_s[0], jnp.where(row8 == 1, ts_s[1], jnp.where(row8 < 6, ts_s[2], 0.0)))

    def inner(g, k):
        arrived(x_s.at[g], load_sem.at[k])
        x_s[g, 0:128, :] = h_raw[pl.ds(g * SPAN, SPAN)].reshape(128, 1024)
        x_s[g, 128:256, :] = g_raw[pl.ds(g * SPAN, SPAN)].reshape(128, 1024)
        left, right = slice(0, 512), slice(512, 1024)
        p1 = mm(x_s[g, :, left], x_s[g, 0:128, left], NT) + mm(x_s[g, :, right], x_s[g, 0:128, right], NT)
        p2 = mm(y_s[g, :, left], x_s[g, 128:256, left], NT) + mm(y_s[g, :, right], x_s[g, 128:256, right], NT)
        square = jnp.sum(jnp.where(same, p1[0:128], 0.0), axis=0, keepdims=True)
        dmix = jnp.sum(jnp.where(token, p1[128:256], 0.0).reshape(16, 8, 128), axis=0)
        dmix = dmix + pltpu.roll(dmix, 4, 0)
        dalpha = jnp.sum(jnp.where(owner, p1[256:288], 0.0), axis=0, keepdims=True)
        dbeta = jnp.sum(jnp.where(owner, p2, 0.0), axis=0, keepdims=True)
        lin = p1[288:296] + p1[296:304] + p1[304:312]
        own_s[g, 0:8, :] = jnp.where(row8 == 6, square, jnp.where(row8 == 7, dbeta, lin))
        own_s[g, 8:13, :] = jnp.where(row8 == 0, dalpha, pltpu.roll(dmix, 1, 0))[0:5]

    def pass_on(k):
        return pltpu.make_async_remote_copy(
            src_ref=own_s.at[order[k]], dst_ref=near_s.at[k],
            send_sem=st_send, recv_sem=near_recv.at[k],
            device_id=tensor_peer(0, 1), device_id_type=pl.DeviceIdType.MESH,
        )

    inner(order[0], 0)
    inner(order[1], 1)
    inner(order[2], 2)
    pl.semaphore_wait(barrier, len(peers))
    pass_on(0).start()
    pass_on(1).start()
    inner(order[3], 3)
    for k in range(2):
        slot = x * GROUPS + order[2 + k]
        pass_on(k).wait_recv()
        stat[slot] = own_s[order[2 + k]] + near_s[k]
        for dx, dc in FAR_X:
            pltpu.make_async_remote_copy(
                src_ref=stat.at[slot], dst_ref=stat.at[slot],
                send_sem=st_send, recv_sem=st_recv.at[k],
                device_id=tensor_peer(dx, dc), device_id_type=pl.DeviceIdType.MESH,
            ).start()

    dw = jnp.zeros((8, 1024), F32)
    for k in range(2):
        arrived(stat.at[pl.ds(0, 7)], st_recv.at[k])
        for i in (2 * k, 2 * k + 1):
            total = (stat[i] + stat[4 + i]) + (stat[8 + i] + stat[12 + i])
            lin = total[0:8]
            dcoef = jnp.concatenate([total[7:13], jnp.zeros((2, 128), F32)], axis=0)
            inv = lax.rsqrt(total[6:7] / D + 1e-06)
            bent = jnp.tanh(inv * lin)
            dpre = dcoef * sv * (1.0 - bent * bent)
            dlin = dpre * inv
            coef_s[i, 0:8, :] = mixv + sv * bent
            coef_s[i, 8:16, :] = dlin
            dsq2 = -1.0 * (inv * inv * inv) / D * jnp.sum(dpre * lin, axis=0, keepdims=True)
            coef_s[i, 16:24, :] = jnp.broadcast_to(dsq2, (8, 128))
            d_hi, d_lo = split(dlin)
            left = jnp.concatenate([d_hi, d_lo], axis=0).astype(BF16)
            part = mm(left, x_s[i, 0:128, :], NN)
            dw = dw + (part[0:8] + part[8:16])

    for q in range(8):
        a, b = q // 4, q % 4
        dw1[a, 6 * b : 6 * b + 6, :] = dw[0:6, 128 * q : 128 * q + 128]

    def give(step, a, source, got, axis):
        own = (yy, zz)[axis]
        for n in range(7):
            pltpu.make_async_remote_copy(
                src_ref=source.at[a], dst_ref=got.at[a, own],
                send_sem=dw_send.at[step], recv_sem=dw_recv.at[step, a],
                device_id=(y_peer, z_peer)[axis](n), device_id_type=pl.DeviceIdType.MESH,
            ).start()
        got[a, own] = source[a]

    def take(step, a, got):
        arrived(got.at[a, pl.ds(0, 7)], dw_recv.at[step, a])
        total = got[a, 0]
        for n in range(1, 8):
            total = total + got[a, n]
        return total

    def grads(i, carry):
        coef, dlin, dsq2 = coef_s[i, 0:8, :], coef_s[i, 8:16, :], coef_s[i, 16:17, :]
        mix8 = jnp.where(row8 < 4, pltpu.roll(coef, 6, 0), pltpu.roll(coef, 2, 0))
        mixer = jnp.where(token, jnp.broadcast_to(mix8[None], (16, 8, 128)).reshape(128, 128), 0.0)
        diag = jnp.where(same, dsq2, 0.0)
        alpha = jnp.where(owner, coef[1:2], 0.0)
        left = jnp.concatenate([diag, mixer, alpha, dlin, dlin, dlin, jnp.zeros_like(dlin)], axis=0)
        high, low = split(left)
        both = jnp.concatenate([high.T, low.T], axis=0).astype(BF16)
        beta = jnp.where(owner, coef[0:1], 0.0)
        b_high, b_low = split(beta)
        b_both = jnp.concatenate([b_high, b_low], axis=0).astype(BF16)
        part = pl.ds(pl.multiple_of(i * SPAN, SPAN), SPAN)
        for n in range(4):
            columns = slice(256 * n, 256 * n + 256)
            out = mm(both, x_s[i, :, columns], NN)
            sg_s[part, :, columns] = (out[0:128] + out[128:256]).astype(BF16).reshape(SPAN, 4, 256)
            out = mm(b_both, x_s[i, 128:256, columns], NN)
            og_s[part, columns] = (out[0:SPAN] + out[SPAN : 2 * SPAN]).astype(BF16)
        return carry

    give(0, 0, dw1, got1, 0)
    give(0, 1, dw1, got1, 1)
    lax.fori_loop(0, 2, grads, 0)
    for a in range(2):
        dw2[a] = take(0, a, got1)
        give(1, a, dw2, got2, 1 - a)
    lax.fori_loop(2, 4, grads, 0)
    sums = [take(1, 0, got2), take(1, 1, got2)]
    per_proj = 1.0 / (4.0 * 64 * 128 * D) ** 0.5
    per_gain = 1.0 / (4.0 * 64 * 128) ** 0.5
    for q in range(8):
        a, b = q // 4, q % 4
        columns = slice(128 * q, 128 * q + 128)
        total = sums[a][6 * b : 6 * b + 6]
        pg_out[:, columns] = gain_s[:, columns] * total * per_proj
        gg_out[:, columns] = jnp.sum(total * proj_s[:, columns], axis=0, keepdims=True) * per_gain
    arrived(stat, st_send)
    arrived(got1.at[:, pl.ds(0, 7)], dw_send.at[0])
    arrived(got2.at[:, pl.ds(0, 7)], dw_send.at[1])


def store(*refs):
    copies = [pltpu.make_async_copy(refs[n], refs[4 + n], refs[8].at[n]) for n in range(4)]
    for copy in copies:
        copy.start()
    for copy in copies:
        copy.wait()


def shards(streams, layer_out, cotangent, input_cot, gain, projection, static_mix, tanh_scale):
    anywhere = pl.BlockSpec(memory_space=pl.ANY)
    vmem = pl.BlockSpec(memory_space=pltpu.VMEM)
    sg, og, pg, gg = pl.pallas_call(
        body,
        out_shape=(
            pltpu.VMEM(streams.shape, BF16),
            pltpu.VMEM(layer_out.shape, BF16),
            pltpu.VMEM((6, 1024), F32),
            pltpu.VMEM((1, 1024), F32),
        ),
        in_specs=[anywhere] * 8,
        out_specs=(vmem,) * 4,
        scratch_shapes=[
            pltpu.VMEM((128, 4, 1024), BF16),
            pltpu.VMEM((128, 4, 1024), BF16),
            pltpu.VMEM((GROUPS, SPAN, 1024), BF16),
            pltpu.VMEM((GROUPS, ROWS, 1024), BF16),
            pltpu.VMEM((1, 1024), F32),
            pltpu.VMEM((6, 1024), F32),
            pltpu.SMEM((4, 6), F32),
            pltpu.SMEM((3,), F32),
            pltpu.VMEM((8, 1024), F32),
            pltpu.VMEM((GROUPS, 13, 128), F32),
            pltpu.VMEM((2, 13, 128), F32),
            pltpu.VMEM((4 * GROUPS, 13, 128), F32),
            pltpu.VMEM((GROUPS, 24, 128), F32),
            pltpu.VMEM((2, 24, 128), F32),
            pltpu.VMEM((2, 24, 128), F32),
            pltpu.VMEM((2, 8, 24, 128), F32),
            pltpu.VMEM((2, 8, 24, 128), F32),
            pltpu.SemaphoreType.DMA((GROUPS,)),
            pltpu.SemaphoreType.DMA((4,)),
            pltpu.SemaphoreType.DMA((2,)),
            pltpu.SemaphoreType.DMA,
            pltpu.SemaphoreType.DMA((2,)),
            pltpu.SemaphoreType.DMA((2,)),
            pltpu.SemaphoreType.DMA((2, 2)),
        ],
        compiler_params=pltpu.CompilerParams(collective_id=0, has_side_effects=True),
    )(streams, layer_out, cotangent, input_cot, gain.reshape(1, 1024), projection, static_mix, tanh_scale)
    made = (sg, og, pg, gg)
    sg, og, pg, gg = pl.pallas_call(
        store,
        out_shape=tuple(jax.ShapeDtypeStruct(a.shape, a.dtype) for a in made),
        in_specs=[vmem] * 4,
        out_specs=(anywhere,) * 4,
        scratch_shapes=[pltpu.SemaphoreType.DMA((4,))],
    )(*(pltpu.with_memory_space_constraint(a, pltpu.VMEM) for a in made))
    return sg, og, pg, gg.reshape(1024)


def solution(mesh):
    placed = (
        P("dp", None, "tensor"),
        P("dp", "tensor"),
        P("dp", None, "tensor"),
        P("dp", "tensor"),
        P("tensor"),
        P(None, "tensor"),
        P(),
        P(),
    )
    return jax.shard_map(
        shards,
        mesh=mesh,
        in_specs=placed,
        out_specs=(P("dp", None, "tensor"), P("dp", "tensor"), P(None, "tensor"), P("tensor")),
        check_vma=False,
    )
```

```python
import functools

import jax
import jax.numpy as jnp
from jax import lax
from jax.experimental import pallas as pl
from jax.experimental.pallas import tpu as pltpu
from jax.sharding import PartitionSpec as P

D = 8192
F32, BF16 = jnp.float32, jnp.bfloat16
NT = (((1,), (1,)), ((), ()))
NN = (((1,), (0,)), ((), ()))
TN = (((0,), (0,)), ((), ()))
GROUPS = 4
SPAN = 32
FAR_X = ((2, 0), (2, 1), (1, 0), (3, 0), (1, 1), (3, 1), (0, 1))
ROWS = 320


def mm(a, b, dims):
    return lax.dot_general(a, b, dims, preferred_element_type=F32)


def split(v):
    high = v.astype(BF16).astype(F32)
    return high, v - high


def body(
    h_hbm, y_hbm, g_hbm, g0_hbm, gain_hbm, proj_hbm, mix_hbm, ts_hbm,
    sg_s, og_s, pg_out, gg_out,
    h_raw, g_raw, y_s, x_s, gain_s, proj_s, mix_s, ts_s, w_s, own_s, near_s, stat, coef_s, dw1, dw2, got1, got2,
    load_sem, small_sem, near_recv, st_send, st_recv, dw_send, dw_recv,
    beside, across, all_in,
):
    dp, tensor = lax.axis_index("dp"), lax.axis_index("tensor")
    x, core = tensor // 2, tensor % 2
    yy, zz = dp // 8, dp % 8

    order = (1 - core, 3 - core, core, 2 + core)

    def loads(k):
        part = pl.ds(pl.multiple_of(order[k] * SPAN, SPAN), SPAN)
        for src, dst in (
            (h_hbm.at[part], h_raw.at[part]),
            (g_hbm.at[part], g_raw.at[part]),
            (g0_hbm.at[part], x_s.at[order[k], pl.ds(256, SPAN)]),
            (y_hbm.at[part], y_s.at[order[k]]),
        ):
            pltpu.make_async_copy(src, dst, load_sem.at[k]).start()

    smalls = [
        pltpu.make_async_copy(src, dst, small_sem.at[n])
        for n, (src, dst) in enumerate(((mix_hbm, mix_s), (ts_hbm, ts_s), (gain_hbm, gain_s), (proj_hbm, proj_s)))
    ]
    for copy in smalls:
        copy.start()
    loads(0)

    def arrived(like, sem):
        pltpu.make_async_copy(like, like, sem).wait()

    def tensor_peer(dx, dc):
        return {"dp": dp, "tensor": ((x + dx) % 4) * 2 + (core + dc) % 2}

    def y_peer(n):
        return {"dp": (n + (n + 8 - yy) // 8) * 8 + zz, "tensor": tensor}

    def z_peer(n):
        return {"dp": yy * 8 + n + (n + 8 - zz) // 8, "tensor": tensor}

    barrier = pltpu.get_barrier_semaphore()
    role = (tensor + 6) % 8

    def signal(sem, peer):
        pl.semaphore_signal(sem, inc=1, device_id=peer, device_id_type=pl.DeviceIdType.MESH)

    def at(n):
        return {"dp": dp, "tensor": (n + 2) % 8}

    for n in range(6):
        signal(barrier, at(n + (n + 7 - role) // 7))

    @pl.when(role == 7)
    def _():
        signal(barrier, at(6))

    for k in range(1, GROUPS):
        loads(k)

    row8 = lax.broadcasted_iota(jnp.int32, (8, 128), 0)
    lane8 = lax.broadcasted_iota(jnp.int32, (8, 128), 1)
    row = lax.broadcasted_iota(jnp.int32, (128, 128), 0)
    lane = lax.broadcasted_iota(jnp.int32, (128, 128), 1)
    same = row == lane
    token = (row // 4) == (lane // 4)
    owner = row[:SPAN] == (lane[:SPAN] // 4)

    for copy in smalls:
        copy.wait()
    w_s[...] = jnp.zeros_like(w_s)
    w_s[0:6, :] = gain_s[...] * proj_s[...]
    w_hi, w_rest = split(w_s[...])
    w_mid, w_lo = split(w_rest)
    w_all = jnp.concatenate([w_hi, w_mid, w_lo, jnp.zeros_like(w_lo)], axis=0).astype(BF16)
    for i in range(GROUPS):
        x_s[i, 288:320, :] = w_all
    mixv = jnp.zeros((8, 128), F32)
    for c in range(6):
        for j in range(4):
            mixv = jnp.where((row8 == c) & (lane8 % 4 == j), mix_s[j, c], mixv)
    sv = jnp.where(row8 == 0, ts_s[0], jnp.where(row8 == 1, ts_s[1], jnp.where(row8 < 6, ts_s[2], 0.0)))

    def inner(g, k):
        arrived(x_s.at[g], load_sem.at[k])
        x_s[g, 0:128, :] = h_raw[pl.ds(g * SPAN, SPAN)].reshape(128, 1024)
        x_s[g, 128:256, :] = g_raw[pl.ds(g * SPAN, SPAN)].reshape(128, 1024)
        left, right = slice(0, 512), slice(512, 1024)
        p1 = mm(x_s[g, :, left], x_s[g, 0:128, left], NT) + mm(x_s[g, :, right], x_s[g, 0:128, right], NT)
        p2 = mm(y_s[g, :, left], x_s[g, 128:256, left], NT) + mm(y_s[g, :, right], x_s[g, 128:256, right], NT)
        square = jnp.sum(jnp.where(same, p1[0:128], 0.0), axis=0, keepdims=True)
        dmix = jnp.sum(jnp.where(token, p1[128:256], 0.0).reshape(16, 8, 128), axis=0)
        dmix = dmix + pltpu.roll(dmix, 4, 0)
        dalpha = jnp.sum(jnp.where(owner, p1[256:288], 0.0), axis=0, keepdims=True)
        dbeta = jnp.sum(jnp.where(owner, p2, 0.0), axis=0, keepdims=True)
        lin = p1[288:296] + p1[296:304] + p1[304:312]
        own_s[g, 0:8, :] = jnp.where(row8 == 6, square, jnp.where(row8 == 7, dbeta, lin))
        own_s[g, 8:13, :] = jnp.where(row8 == 0, dalpha, pltpu.roll(dmix, 1, 0))[0:5]

    def pass_on(k):
        return pltpu.make_async_remote_copy(
            src_ref=own_s.at[order[k]], dst_ref=near_s.at[k],
            send_sem=st_send, recv_sem=near_recv.at[k],
            device_id=tensor_peer(0, 1), device_id_type=pl.DeviceIdType.MESH,
        )

    inner(order[0], 0)
    @pl.when(role < 7)
    def _():
        pl.semaphore_wait(barrier, 7)

    @pl.when(role == 6)
    def _():
        signal(beside, at(7))
        for n in range(7):
            for peer in (y_peer, z_peer):
                signal(barrier, {"dp": peer(n)["dp"], "tensor": 1})

    @pl.when(role < 6)
    def _():
        signal(across, at(7))

    def tell(k):
        slot = x * GROUPS + order[2 + k]
        pass_on(k).wait_recv()
        stat[slot] = own_s[order[2 + k]] + near_s[k]
        for dx, dc in FAR_X:
            pltpu.make_async_remote_copy(
                src_ref=stat.at[slot], dst_ref=stat.at[slot],
                send_sem=st_send, recv_sem=st_recv.at[k],
                device_id=tensor_peer(dx, dc), device_id_type=pl.DeviceIdType.MESH,
            ).start()

    @pl.when(role == 7)
    def _():
        pl.semaphore_wait(beside, 1)

    pass_on(0).start()
    inner(order[1], 1)
    pass_on(1).start()
    inner(order[2], 2)

    @pl.when(role == 7)
    def _():
        pl.semaphore_wait(across, 6)

    tell(0)
    inner(order[3], 3)
    tell(1)

    @pl.when(role == 7)
    def _():
        pl.semaphore_wait(barrier, 14)
        for n in range(7):
            signal(all_in, at(n))

    dw = jnp.zeros((8, 1024), F32)
    for k in range(2):
        arrived(stat.at[pl.ds(0, 7)], st_recv.at[k])
        for i in (2 * k, 2 * k + 1):
            total = (stat[i] + stat[4 + i]) + (stat[8 + i] + stat[12 + i])
            lin = total[0:8]
            dcoef = jnp.concatenate([total[7:13], jnp.zeros((2, 128), F32)], axis=0)
            inv = lax.rsqrt(total[6:7] / D + 1e-06)
            bent = jnp.tanh(inv * lin)
            dpre = dcoef * sv * (1.0 - bent * bent)
            dlin = dpre * inv
            coef_s[i, 0:8, :] = mixv + sv * bent
            coef_s[i, 8:16, :] = dlin
            dsq2 = -1.0 * (inv * inv * inv) / D * jnp.sum(dpre * lin, axis=0, keepdims=True)
            coef_s[i, 16:24, :] = jnp.broadcast_to(dsq2, (8, 128))
            d_hi, d_lo = split(dlin)
            left = jnp.concatenate([d_hi, d_lo], axis=0).astype(BF16)
            part = mm(left, x_s[i, 0:128, :], NN)
            dw = dw + (part[0:8] + part[8:16])

    for q in range(8):
        a, b = q // 4, q % 4
        dw1[a, 6 * b : 6 * b + 6, :] = dw[0:6, 128 * q : 128 * q + 128]

    def give(step, a, source, got, axis):
        own = (yy, zz)[axis]
        for n in range(7):
            pltpu.make_async_remote_copy(
                src_ref=source.at[a], dst_ref=got.at[a, own],
                send_sem=dw_send.at[step], recv_sem=dw_recv.at[step, a],
                device_id=(y_peer, z_peer)[axis](n), device_id_type=pl.DeviceIdType.MESH,
            ).start()
        got[a, own] = source[a]

    def take(step, a, got):
        arrived(got.at[a, pl.ds(0, 7)], dw_recv.at[step, a])
        total = got[a, 0]
        for n in range(1, 8):
            total = total + got[a, n]
        return total

    def grads(i, carry):
        coef, dlin, dsq2 = coef_s[i, 0:8, :], coef_s[i, 8:16, :], coef_s[i, 16:17, :]
        mix8 = jnp.where(row8 < 4, pltpu.roll(coef, 6, 0), pltpu.roll(coef, 2, 0))
        mixer = jnp.where(token, jnp.broadcast_to(mix8[None], (16, 8, 128)).reshape(128, 128), 0.0)
        diag = jnp.where(same, dsq2, 0.0)
        alpha = jnp.where(owner, coef[1:2], 0.0)
        left = jnp.concatenate([diag, mixer, alpha, dlin, dlin, dlin, jnp.zeros_like(dlin)], axis=0)
        high, low = split(left)
        both = jnp.concatenate([high.T, low.T], axis=0).astype(BF16)
        beta = jnp.where(owner, coef[0:1], 0.0)
        b_high, b_low = split(beta)
        b_both = jnp.concatenate([b_high, b_low], axis=0).astype(BF16)
        part = pl.ds(pl.multiple_of(i * SPAN, SPAN), SPAN)
        for n in range(4):
            columns = slice(256 * n, 256 * n + 256)
            out = mm(both, x_s[i, :, columns], NN)
            sg_s[part, :, columns] = (out[0:128] + out[128:256]).astype(BF16).reshape(SPAN, 4, 256)
            out = mm(b_both, x_s[i, 128:256, columns], NN)
            og_s[part, columns] = (out[0:SPAN] + out[SPAN : 2 * SPAN]).astype(BF16)
        return carry


    @pl.when(role < 7)
    def _():
        pl.semaphore_wait(all_in, 1)

    give(0, 0, dw1, got1, 0)
    give(0, 1, dw1, got1, 1)
    lax.fori_loop(0, 2, grads, 0)
    for a in range(2):
        dw2[a] = take(0, a, got1)
        give(1, a, dw2, got2, 1 - a)
    lax.fori_loop(2, 4, grads, 0)
    sums = [take(1, 0, got2), take(1, 1, got2)]
    per_proj = 1.0 / (4.0 * 64 * 128 * D) ** 0.5
    per_gain = 1.0 / (4.0 * 64 * 128) ** 0.5
    for q in range(8):
        a, b = q // 4, q % 4
        columns = slice(128 * q, 128 * q + 128)
        total = sums[a][6 * b : 6 * b + 6]
        pg_out[:, columns] = gain_s[:, columns] * total * per_proj
        gg_out[:, columns] = jnp.sum(total * proj_s[:, columns], axis=0, keepdims=True) * per_gain
    arrived(stat, st_send)
    arrived(got1.at[:, pl.ds(0, 7)], dw_send.at[0])
    arrived(got2.at[:, pl.ds(0, 7)], dw_send.at[1])


def store(*refs):
    copies = [pltpu.make_async_copy(refs[n], refs[4 + n], refs[8].at[n]) for n in range(4)]
    for copy in copies:
        copy.start()
    for copy in copies:
        copy.wait()


def shards(streams, layer_out, cotangent, input_cot, gain, projection, static_mix, tanh_scale):
    anywhere = pl.BlockSpec(memory_space=pl.ANY)
    vmem = pl.BlockSpec(memory_space=pltpu.VMEM)
    sg, og, pg, gg = pl.pallas_call(
        body,
        out_shape=(
            pltpu.VMEM(streams.shape, BF16),
            pltpu.VMEM(layer_out.shape, BF16),
            pltpu.VMEM((6, 1024), F32),
            pltpu.VMEM((1, 1024), F32),
        ),
        in_specs=[anywhere] * 8,
        out_specs=(vmem,) * 4,
        scratch_shapes=[
            pltpu.VMEM((128, 4, 1024), BF16),
            pltpu.VMEM((128, 4, 1024), BF16),
            pltpu.VMEM((GROUPS, SPAN, 1024), BF16),
            pltpu.VMEM((GROUPS, ROWS, 1024), BF16),
            pltpu.VMEM((1, 1024), F32),
            pltpu.VMEM((6, 1024), F32),
            pltpu.SMEM((4, 6), F32),
            pltpu.SMEM((3,), F32),
            pltpu.VMEM((8, 1024), F32),
            pltpu.VMEM((GROUPS, 13, 128), F32),
            pltpu.VMEM((2, 13, 128), F32),
            pltpu.VMEM((4 * GROUPS, 13, 128), F32),
            pltpu.VMEM((GROUPS, 24, 128), F32),
            pltpu.VMEM((2, 24, 128), F32),
            pltpu.VMEM((2, 24, 128), F32),
            pltpu.VMEM((2, 8, 24, 128), F32),
            pltpu.VMEM((2, 8, 24, 128), F32),
            pltpu.SemaphoreType.DMA((GROUPS,)),
            pltpu.SemaphoreType.DMA((4,)),
            pltpu.SemaphoreType.DMA((2,)),
            pltpu.SemaphoreType.DMA,
            pltpu.SemaphoreType.DMA((2,)),
            pltpu.SemaphoreType.DMA((2,)),
            pltpu.SemaphoreType.DMA((2, 2)),
            pltpu.SemaphoreType.REGULAR,
            pltpu.SemaphoreType.REGULAR,
            pltpu.SemaphoreType.REGULAR,
        ],
        compiler_params=pltpu.CompilerParams(collective_id=0, has_side_effects=True),
    )(streams, layer_out, cotangent, input_cot, gain.reshape(1, 1024), projection, static_mix, tanh_scale)
    made = (sg, og, pg, gg)
    sg, og, pg, gg = pl.pallas_call(
        store,
        out_shape=tuple(jax.ShapeDtypeStruct(a.shape, a.dtype) for a in made),
        in_specs=[vmem] * 4,
        out_specs=(anywhere,) * 4,
        scratch_shapes=[pltpu.SemaphoreType.DMA((4,))],
    )(*(pltpu.with_memory_space_constraint(a, pltpu.VMEM) for a in made))
    return sg, og, pg, gg.reshape(1024)


def solution(mesh):
    placed = (
        P("dp", None, "tensor"),
        P("dp", "tensor"),
        P("dp", None, "tensor"),
        P("dp", "tensor"),
        P("tensor"),
        P(None, "tensor"),
        P(),
        P(),
    )
    return jax.shard_map(
        shards,
        mesh=mesh,
        in_specs=placed,
        out_specs=(P("dp", None, "tensor"), P("dp", "tensor"), P(None, "tensor"), P("tensor")),
        check_vma=False,
    )
```

```python
import functools

import jax
import jax.numpy as jnp
from jax import lax
from jax.experimental import pallas as pl
from jax.experimental.pallas import tpu as pltpu
from jax.sharding import PartitionSpec as P

D = 8192
F32, BF16 = jnp.float32, jnp.bfloat16
NT = (((1,), (1,)), ((), ()))
NN = (((1,), (0,)), ((), ()))
TN = (((0,), (0,)), ((), ()))
GROUPS = 4
SPAN = 32
FAR_X = ((2, 0), (2, 1), (1, 0), (3, 0), (1, 1), (3, 1), (0, 1))
ROWS = 320


def mm(a, b, dims):
    return lax.dot_general(a, b, dims, preferred_element_type=F32)


def split(v):
    high = v.astype(BF16).astype(F32)
    return high, v - high


def body(
    h_hbm, y_hbm, g_hbm, g0_hbm, gain_hbm, proj_hbm, mix_hbm, ts_hbm,
    sg_s, og_s, pg_out, gg_out,
    h_raw, g_raw, y_s, x_s, gain_s, proj_s, mix_s, ts_s, w_s, own_s, near_s, stat, coef_s, dw1, dw2, got1, got2,
    load_sem, small_sem, near_recv, st_send, st_recv, dw_send, dw_recv,
    beside, across, all_in,
):
    dp, tensor = lax.axis_index("dp"), lax.axis_index("tensor")
    x, core = tensor // 2, tensor % 2
    yy, zz = dp // 8, dp % 8

    order = (1 - core, 3 - core, core, 2 + core)

    def loads(k):
        part = pl.ds(pl.multiple_of(order[k] * SPAN, SPAN), SPAN)
        for src, dst in (
            (h_hbm.at[part], h_raw.at[k]),
            (g_hbm.at[part], g_raw.at[k]),
            (g0_hbm.at[part], x_s.at[k, pl.ds(256, SPAN)]),
            (y_hbm.at[part], y_s.at[k]),
        ):
            pltpu.make_async_copy(src, dst, load_sem.at[k]).start()

    smalls = [
        pltpu.make_async_copy(src, dst, small_sem.at[n])
        for n, (src, dst) in enumerate(((mix_hbm, mix_s), (ts_hbm, ts_s), (gain_hbm, gain_s), (proj_hbm, proj_s)))
    ]
    for copy in smalls:
        copy.start()
    loads(0)

    def arrived(like, sem):
        pltpu.make_async_copy(like, like, sem).wait()

    def tensor_peer(dx, dc):
        return {"dp": dp, "tensor": ((x + dx) % 4) * 2 + (core + dc) % 2}

    def y_peer(n):
        return {"dp": (n + (n + 8 - yy) // 8) * 8 + zz, "tensor": tensor}

    def z_peer(n):
        return {"dp": yy * 8 + n + (n + 8 - zz) // 8, "tensor": tensor}

    barrier = pltpu.get_barrier_semaphore()
    role = (tensor + 6) % 8

    def signal(sem, peer):
        pl.semaphore_signal(sem, inc=1, device_id=peer, device_id_type=pl.DeviceIdType.MESH)

    def at(n):
        return {"dp": dp, "tensor": (n + 2) % 8}

    for n in range(6):
        signal(barrier, at(n + (n + 7 - role) // 7))

    @pl.when(role == 7)
    def _():
        signal(barrier, at(6))

    for k in range(1, GROUPS):
        loads(k)

    row8 = lax.broadcasted_iota(jnp.int32, (8, 128), 0)
    lane8 = lax.broadcasted_iota(jnp.int32, (8, 128), 1)
    row = lax.broadcasted_iota(jnp.int32, (128, 128), 0)
    lane = lax.broadcasted_iota(jnp.int32, (128, 128), 1)
    same = row == lane
    token = (row // 4) == (lane // 4)
    owner = row[:SPAN] == (lane[:SPAN] // 4)

    for copy in smalls:
        copy.wait()
    w_s[...] = jnp.zeros_like(w_s)
    w_s[0:6, :] = gain_s[...] * proj_s[...]
    w_hi, w_rest = split(w_s[...])
    w_mid, w_lo = split(w_rest)
    w_all = jnp.concatenate([w_hi, w_mid, w_lo, jnp.zeros_like(w_lo)], axis=0).astype(BF16)
    for i in range(GROUPS):
        x_s[i, 288:320, :] = w_all
    mixv = jnp.zeros((8, 128), F32)
    for c in range(6):
        for j in range(4):
            mixv = jnp.where((row8 == c) & (lane8 % 4 == j), mix_s[j, c], mixv)
    sv = jnp.where(row8 == 0, ts_s[0], jnp.where(row8 == 1, ts_s[1], jnp.where(row8 < 6, ts_s[2], 0.0)))

    def inner(k):
        x_s[k, 0:128, :] = h_raw[k].reshape(128, 1024)
        x_s[k, 128:256, :] = g_raw[k].reshape(128, 1024)
        p1 = mm(x_s[k], x_s[k, 0:128, :], NT)
        p2 = mm(y_s[k], x_s[k, 128:256, :], NT)
        square = jnp.sum(jnp.where(same, p1[0:128], 0.0), axis=0, keepdims=True)
        dmix = jnp.sum(jnp.where(token, p1[128:256], 0.0).reshape(16, 8, 128), axis=0)
        dmix = dmix + pltpu.roll(dmix, 4, 0)
        dalpha = jnp.sum(jnp.where(owner, p1[256:288], 0.0), axis=0, keepdims=True)
        dbeta = jnp.sum(jnp.where(owner, p2, 0.0), axis=0, keepdims=True)
        lin = p1[288:296] + p1[296:304] + p1[304:312]
        own_s[k, 0:8, :] = jnp.where(row8 == 6, square, jnp.where(row8 == 7, dbeta, lin))
        own_s[k, 8:13, :] = jnp.where(row8 == 0, dalpha, pltpu.roll(dmix, 1, 0))[0:5]

    def pass_on(k):
        return pltpu.make_async_remote_copy(
            src_ref=own_s.at[k], dst_ref=near_s.at[k],
            send_sem=st_send, recv_sem=near_recv.at[k],
            device_id=tensor_peer(0, 1), device_id_type=pl.DeviceIdType.MESH,
        )

    def pair(k):
        for n in (k, k + 1):
            arrived(x_s.at[n], load_sem.at[n])
        inner(k)
        inner(k + 1)

    pair(0)

    @pl.when(role < 7)
    def _():
        pl.semaphore_wait(barrier, 7)

    @pl.when(role == 6)
    def _():
        signal(beside, at(7))
        for n in range(7):
            for peer in (y_peer, z_peer):
                signal(barrier, {"dp": peer(n)["dp"], "tensor": 1})

    @pl.when(role < 6)
    def _():
        signal(across, at(7))

    def tell(k):
        slot = x * GROUPS + order[2 + k]
        pass_on(k).wait_recv()
        stat[slot] = own_s[2 + k] + near_s[k]
        for dx, dc in FAR_X:
            pltpu.make_async_remote_copy(
                src_ref=stat.at[slot], dst_ref=stat.at[slot],
                send_sem=st_send, recv_sem=st_recv.at[k],
                device_id=tensor_peer(dx, dc), device_id_type=pl.DeviceIdType.MESH,
            ).start()

    @pl.when(role < 7)
    def _():
        pass_on(0).start()
        pass_on(1).start()

    pair(2)

    @pl.when(role == 7)
    def _():
        pl.semaphore_wait(beside, 1)
        pass_on(0).start()
        pass_on(1).start()
        pl.semaphore_wait(across, 6)

    tell(0)
    tell(1)

    @pl.when(role == 7)
    def _():
        pl.semaphore_wait(barrier, 14)
        for n in range(7):
            signal(all_in, at(n))

    dw = jnp.zeros((8, 1024), F32)
    for k in range(2):
        arrived(stat.at[pl.ds(0, 7)], st_recv.at[k])
        for i in (k, k + 2):
            g = order[i]
            total = (stat[g] + stat[4 + g]) + (stat[8 + g] + stat[12 + g])
            lin = total[0:8]
            dcoef = jnp.concatenate([total[7:13], jnp.zeros((2, 128), F32)], axis=0)
            inv = lax.rsqrt(total[6:7] / D + 1e-06)
            bent = jnp.tanh(inv * lin)
            dpre = dcoef * sv * (1.0 - bent * bent)
            dlin = dpre * inv
            coef_s[i, 0:8, :] = mixv + sv * bent
            coef_s[i, 8:16, :] = dlin
            dsq2 = -1.0 * (inv * inv * inv) / D * jnp.sum(dpre * lin, axis=0, keepdims=True)
            coef_s[i, 16:24, :] = jnp.broadcast_to(dsq2, (8, 128))
            d_hi, d_lo = split(dlin)
            left = jnp.concatenate([d_hi, d_lo], axis=0).astype(BF16)
            part = mm(left, x_s[i, 0:128, :], NN)
            dw = dw + (part[0:8] + part[8:16])

    for q in range(8):
        a, b = q // 4, q % 4
        dw1[a, 6 * b : 6 * b + 6, :] = dw[0:6, 128 * q : 128 * q + 128]

    def give(step, a, source, got, axis):
        own = (yy, zz)[axis]
        for n in range(7):
            pltpu.make_async_remote_copy(
                src_ref=source.at[a], dst_ref=got.at[a, own],
                send_sem=dw_send.at[step], recv_sem=dw_recv.at[step, a],
                device_id=(y_peer, z_peer)[axis](n), device_id_type=pl.DeviceIdType.MESH,
            ).start()
        got[a, own] = source[a]

    def take(step, a, got):
        arrived(got.at[a, pl.ds(0, 7)], dw_recv.at[step, a])
        total = got[a, 0]
        for n in range(1, 8):
            total = total + got[a, n]
        return total

    def grads(i, carry):
        coef, dlin, dsq2 = coef_s[i, 0:8, :], coef_s[i, 8:16, :], coef_s[i, 16:17, :]
        mix8 = jnp.where(row8 < 4, pltpu.roll(coef, 6, 0), pltpu.roll(coef, 2, 0))
        mixer = jnp.where(token, jnp.broadcast_to(mix8[None], (16, 8, 128)).reshape(128, 128), 0.0)
        diag = jnp.where(same, dsq2, 0.0)
        alpha = jnp.where(owner, coef[1:2], 0.0)
        left = jnp.concatenate([diag, mixer, alpha, dlin, dlin, dlin, jnp.zeros_like(dlin)], axis=0)
        high, low = split(left)
        both = jnp.concatenate([high.T, low.T], axis=0).astype(BF16)
        beta = jnp.where(owner, coef[0:1], 0.0)
        b_high, b_low = split(beta)
        b_both = jnp.concatenate([b_high, b_low], axis=0).astype(BF16)
        g = 2 * (i % 2) + (i // 2) * core + (1 - i // 2) * (1 - core)
        part = pl.ds(pl.multiple_of(g * SPAN, SPAN), SPAN)
        for n in range(4):
            columns = slice(256 * n, 256 * n + 256)
            out = mm(both, x_s[i, :, columns], NN)
            sg_s[part, :, columns] = (out[0:128] + out[128:256]).astype(BF16).reshape(SPAN, 4, 256)
            out = mm(b_both, x_s[i, 128:256, columns], NN)
            og_s[part, columns] = (out[0:SPAN] + out[SPAN : 2 * SPAN]).astype(BF16)
        return carry


    @pl.when(role < 7)
    def _():
        pl.semaphore_wait(all_in, 1)

    give(0, 0, dw1, got1, 0)
    give(0, 1, dw1, got1, 1)
    lax.fori_loop(0, 2, grads, 0)
    for a in range(2):
        dw2[a] = take(0, a, got1)
        give(1, a, dw2, got2, 1 - a)
    lax.fori_loop(2, 4, grads, 0)
    sums = [take(1, 0, got2), take(1, 1, got2)]
    per_proj = 1.0 / (4.0 * 64 * 128 * D) ** 0.5
    per_gain = 1.0 / (4.0 * 64 * 128) ** 0.5
    for q in range(8):
        a, b = q // 4, q % 4
        columns = slice(128 * q, 128 * q + 128)
        total = sums[a][6 * b : 6 * b + 6]
        pg_out[:, columns] = gain_s[:, columns] * total * per_proj
        gg_out[:, columns] = jnp.sum(total * proj_s[:, columns], axis=0, keepdims=True) * per_gain
    arrived(stat, st_send)
    arrived(got1.at[:, pl.ds(0, 7)], dw_send.at[0])
    arrived(got2.at[:, pl.ds(0, 7)], dw_send.at[1])


def store(*refs):
    copies = [pltpu.make_async_copy(refs[n], refs[4 + n], refs[8].at[n]) for n in range(4)]
    for copy in copies:
        copy.start()
    for copy in copies:
        copy.wait()


def shards(streams, layer_out, cotangent, input_cot, gain, projection, static_mix, tanh_scale):
    anywhere = pl.BlockSpec(memory_space=pl.ANY)
    vmem = pl.BlockSpec(memory_space=pltpu.VMEM)
    sg, og, pg, gg = pl.pallas_call(
        body,
        out_shape=(
            pltpu.VMEM(streams.shape, BF16),
            pltpu.VMEM(layer_out.shape, BF16),
            pltpu.VMEM((6, 1024), F32),
            pltpu.VMEM((1, 1024), F32),
        ),
        in_specs=[anywhere] * 8,
        out_specs=(vmem,) * 4,
        scratch_shapes=[
            pltpu.VMEM((GROUPS, SPAN, 4, 1024), BF16),
            pltpu.VMEM((GROUPS, SPAN, 4, 1024), BF16),
            pltpu.VMEM((GROUPS, SPAN, 1024), BF16),
            pltpu.VMEM((GROUPS, ROWS, 1024), BF16),
            pltpu.VMEM((1, 1024), F32),
            pltpu.VMEM((6, 1024), F32),
            pltpu.SMEM((4, 6), F32),
            pltpu.SMEM((3,), F32),
            pltpu.VMEM((8, 1024), F32),
            pltpu.VMEM((GROUPS, 13, 128), F32),
            pltpu.VMEM((2, 13, 128), F32),
            pltpu.VMEM((4 * GROUPS, 13, 128), F32),
            pltpu.VMEM((GROUPS, 24, 128), F32),
            pltpu.VMEM((2, 24, 128), F32),
            pltpu.VMEM((2, 24, 128), F32),
            pltpu.VMEM((2, 8, 24, 128), F32),
            pltpu.VMEM((2, 8, 24, 128), F32),
            pltpu.SemaphoreType.DMA((GROUPS,)),
            pltpu.SemaphoreType.DMA((4,)),
            pltpu.SemaphoreType.DMA((2,)),
            pltpu.SemaphoreType.DMA,
            pltpu.SemaphoreType.DMA((2,)),
            pltpu.SemaphoreType.DMA((2,)),
            pltpu.SemaphoreType.DMA((2, 2)),
            pltpu.SemaphoreType.REGULAR,
            pltpu.SemaphoreType.REGULAR,
            pltpu.SemaphoreType.REGULAR,
        ],
        compiler_params=pltpu.CompilerParams(collective_id=0, has_side_effects=True),
    )(streams, layer_out, cotangent, input_cot, gain.reshape(1, 1024), projection, static_mix, tanh_scale)
    made = (sg, og, pg, gg)
    sg, og, pg, gg = pl.pallas_call(
        store,
        out_shape=tuple(jax.ShapeDtypeStruct(a.shape, a.dtype) for a in made),
        in_specs=[vmem] * 4,
        out_specs=(anywhere,) * 4,
        scratch_shapes=[pltpu.SemaphoreType.DMA((4,))],
    )(*(pltpu.with_memory_space_constraint(a, pltpu.VMEM) for a in made))
    return sg, og, pg, gg.reshape(1024)


def solution(mesh):
    placed = (
        P("dp", None, "tensor"),
        P("dp", "tensor"),
        P("dp", None, "tensor"),
        P("dp", "tensor"),
        P("tensor"),
        P(None, "tensor"),
        P(),
        P(),
    )
    return jax.shard_map(
        shards,
        mesh=mesh,
        in_specs=placed,
        out_specs=(P("dp", None, "tensor"), P("dp", "tensor"), P(None, "tensor"), P("tensor")),
        check_vma=False,
    )
```

```python
import functools

import jax
import jax.numpy as jnp
from jax import lax
from jax.experimental import pallas as pl
from jax.experimental.pallas import tpu as pltpu
from jax.sharding import PartitionSpec as P

D = 8192
F32, BF16 = jnp.float32, jnp.bfloat16
NT = (((1,), (1,)), ((), ()))
NN = (((1,), (0,)), ((), ()))
TN = (((0,), (0,)), ((), ()))
GROUPS = 4
SPAN = 32
FAR_X = ((2, 0), (2, 1), (1, 0), (3, 0), (1, 1), (3, 1), (0, 1))
ROWS = 320


def mm(a, b, dims):
    return lax.dot_general(a, b, dims, preferred_element_type=F32)


def split(v):
    high = v.astype(BF16).astype(F32)
    return high, v - high


def body(
    h_hbm, y_hbm, g_hbm, g0_hbm, gain_hbm, proj_hbm, mix_hbm, ts_hbm,
    sg_s, og_s, pg_out, gg_out,
    h_raw, g_raw, y_s, x_s, gain_s, proj_s, mix_s, ts_s, w_s, own_s, near_s, stat, coef_s, dw1, dw2, got1, got2,
    load_sem, small_sem, near_recv, st_send, st_recv, dw_send, dw_recv,
    beside, across, all_in,
):
    dp, tensor = lax.axis_index("dp"), lax.axis_index("tensor")
    x, core = tensor // 2, tensor % 2
    yy, zz = dp // 8, dp % 8

    order = (1 - core, 3 - core, core, 2 + core)

    def loads(k):
        part = pl.ds(pl.multiple_of(order[k] * SPAN, SPAN), SPAN)
        for src, dst in (
            (h_hbm.at[part], h_raw.at[k]),
            (g_hbm.at[part], g_raw.at[k]),
            (g0_hbm.at[part], x_s.at[k, pl.ds(256, SPAN)]),
            (y_hbm.at[part], y_s.at[k]),
        ):
            pltpu.make_async_copy(src, dst, load_sem.at[k // 2]).start()

    smalls = [
        pltpu.make_async_copy(src, dst, small_sem.at[n])
        for n, (src, dst) in enumerate(((mix_hbm, mix_s), (ts_hbm, ts_s), (gain_hbm, gain_s), (proj_hbm, proj_s)))
    ]
    for copy in smalls:
        copy.start()
    loads(0)

    def arrived(like, sem):
        pltpu.make_async_copy(like, like, sem).wait()

    def tensor_peer(dx, dc):
        return {"dp": dp, "tensor": ((x + dx) % 4) * 2 + (core + dc) % 2}

    def y_peer(n):
        return {"dp": (n + (n + 8 - yy) // 8) * 8 + zz, "tensor": tensor}

    def z_peer(n):
        return {"dp": yy * 8 + n + (n + 8 - zz) // 8, "tensor": tensor}

    barrier = pltpu.get_barrier_semaphore()
    role = (tensor + 6) % 8

    def signal(sem, peer):
        pl.semaphore_signal(sem, inc=1, device_id=peer, device_id_type=pl.DeviceIdType.MESH)

    def at(n):
        return {"dp": dp, "tensor": (n + 2) % 8}

    for n in range(6):
        signal(barrier, at(n + (n + 7 - role) // 7))

    @pl.when(role == 7)
    def _():
        signal(barrier, at(6))

    for k in range(1, GROUPS):
        loads(k)

    row8 = lax.broadcasted_iota(jnp.int32, (8, 128), 0)
    lane8 = lax.broadcasted_iota(jnp.int32, (8, 128), 1)
    row = lax.broadcasted_iota(jnp.int32, (128, 128), 0)
    lane = lax.broadcasted_iota(jnp.int32, (128, 128), 1)
    same = row == lane
    token = (row // 4) == (lane // 4)
    owner = row[:SPAN] == (lane[:SPAN] // 4)

    for copy in smalls:
        copy.wait()
    w_s[...] = jnp.zeros_like(w_s)
    w_s[0:6, :] = gain_s[...] * proj_s[...]
    w_hi, w_rest = split(w_s[...])
    w_mid, w_lo = split(w_rest)
    w_all = jnp.concatenate([w_hi, w_mid, w_lo, jnp.zeros_like(w_lo)], axis=0).astype(BF16)
    for i in range(GROUPS):
        x_s[i, 288:320, :] = w_all
    mixv = jnp.zeros((8, 128), F32)
    for c in range(6):
        for j in range(4):
            mixv = jnp.where((row8 == c) & (lane8 % 4 == j), mix_s[j, c], mixv)
    sv = jnp.where(row8 == 0, ts_s[0], jnp.where(row8 == 1, ts_s[1], jnp.where(row8 < 6, ts_s[2], 0.0)))

    def inner(k):
        x_s[k, 0:128, :] = h_raw[k].reshape(128, 1024)
        x_s[k, 128:256, :] = g_raw[k].reshape(128, 1024)
        p1 = mm(x_s[k], x_s[k, 0:128, :], NT)
        p2 = mm(y_s[k], x_s[k, 128:256, :], NT)
        square = jnp.sum(jnp.where(same, p1[0:128], 0.0), axis=0, keepdims=True)
        dmix = jnp.sum(jnp.where(token, p1[128:256], 0.0).reshape(16, 8, 128), axis=0)
        dmix = dmix + pltpu.roll(dmix, 4, 0)
        dalpha = jnp.sum(jnp.where(owner, p1[256:288], 0.0), axis=0, keepdims=True)
        dbeta = jnp.sum(jnp.where(owner, p2, 0.0), axis=0, keepdims=True)
        lin = p1[288:296] + p1[296:304] + p1[304:312]
        own_s[k, 0:8, :] = jnp.where(row8 == 6, square, jnp.where(row8 == 7, dbeta, lin))
        own_s[k, 8:13, :] = jnp.where(row8 == 0, dalpha, pltpu.roll(dmix, 1, 0))[0:5]

    def pass_on(k):
        return pltpu.make_async_remote_copy(
            src_ref=own_s.at[k], dst_ref=near_s.at[k],
            send_sem=st_send, recv_sem=near_recv.at[k],
            device_id=tensor_peer(0, 1), device_id_type=pl.DeviceIdType.MESH,
        )

    def pair(k):
        arrived(x_s.at[pl.ds(k, 2)], load_sem.at[k // 2])
        inner(k)
        inner(k + 1)

    pair(0)

    @pl.when(role < 7)
    def _():
        pl.semaphore_wait(barrier, 7)

    @pl.when(role == 6)
    def _():
        signal(beside, at(7))
        for n in range(7):
            for peer in (y_peer, z_peer):
                signal(barrier, {"dp": peer(n)["dp"], "tensor": 1})

    @pl.when(role < 6)
    def _():
        signal(across, at(7))

    def tell(k):
        slot = x * GROUPS + order[2 + k]
        pass_on(k).wait_recv()
        stat[slot] = own_s[2 + k] + near_s[k]
        for dx, dc in FAR_X:
            pltpu.make_async_remote_copy(
                src_ref=stat.at[slot], dst_ref=stat.at[slot],
                send_sem=st_send, recv_sem=st_recv.at[k],
                device_id=tensor_peer(dx, dc), device_id_type=pl.DeviceIdType.MESH,
            ).start()

    @pl.when(role < 7)
    def _():
        pass_on(0).start()
        pass_on(1).start()

    pair(2)

    @pl.when(role == 7)
    def _():
        pl.semaphore_wait(beside, 1)
        pass_on(0).start()
        pass_on(1).start()
        pl.semaphore_wait(across, 6)

    tell(0)
    tell(1)

    @pl.when(role == 7)
    def _():
        pl.semaphore_wait(barrier, 14)
        for n in range(7):
            signal(all_in, at(n))

    dw = jnp.zeros((8, 1024), F32)
    for k in range(2):
        arrived(stat.at[pl.ds(0, 7)], st_recv.at[k])
        for i in (k, k + 2):
            g = order[i]
            total = (stat[g] + stat[4 + g]) + (stat[8 + g] + stat[12 + g])
            lin = total[0:8]
            dcoef = jnp.concatenate([total[7:13], jnp.zeros((2, 128), F32)], axis=0)
            inv = lax.rsqrt(total[6:7] / D + 1e-06)
            bent = jnp.tanh(inv * lin)
            dpre = dcoef * sv * (1.0 - bent * bent)
            dlin = dpre * inv
            coef_s[i, 0:8, :] = mixv + sv * bent
            coef_s[i, 8:16, :] = dlin
            dsq2 = -1.0 * (inv * inv * inv) / D * jnp.sum(dpre * lin, axis=0, keepdims=True)
            coef_s[i, 16:24, :] = jnp.broadcast_to(dsq2, (8, 128))
            d_hi, d_lo = split(dlin)
            left = jnp.concatenate([d_hi, d_lo], axis=0).astype(BF16)
            part = mm(left, x_s[i, 0:128, :], NN)
            dw = dw + (part[0:8] + part[8:16])

    for q in range(8):
        a, b = q // 4, q % 4
        dw1[a, 6 * b : 6 * b + 6, :] = dw[0:6, 128 * q : 128 * q + 128]

    def give(step, a, source, got, axis):
        own = (yy, zz)[axis]
        for n in range(7):
            pltpu.make_async_remote_copy(
                src_ref=source.at[a], dst_ref=got.at[a, own],
                send_sem=dw_send.at[step], recv_sem=dw_recv.at[step, a],
                device_id=(y_peer, z_peer)[axis](n), device_id_type=pl.DeviceIdType.MESH,
            ).start()
        got[a, own] = source[a]

    def take(step, a, got):
        arrived(got.at[a, pl.ds(0, 7)], dw_recv.at[step, a])
        total = got[a, 0]
        for n in range(1, 8):
            total = total + got[a, n]
        return total

    def grads(i, carry):
        coef, dlin, dsq2 = coef_s[i, 0:8, :], coef_s[i, 8:16, :], coef_s[i, 16:17, :]
        mix8 = jnp.where(row8 < 4, pltpu.roll(coef, 6, 0), pltpu.roll(coef, 2, 0))
        mixer = jnp.where(token, jnp.broadcast_to(mix8[None], (16, 8, 128)).reshape(128, 128), 0.0)
        diag = jnp.where(same, dsq2, 0.0)
        alpha = jnp.where(owner, coef[1:2], 0.0)
        left = jnp.concatenate([diag, mixer, alpha, dlin, dlin, dlin, jnp.zeros_like(dlin)], axis=0)
        high, low = split(left)
        both = jnp.concatenate([high.T, low.T], axis=0).astype(BF16)
        beta = jnp.where(owner, coef[0:1], 0.0)
        b_high, b_low = split(beta)
        b_both = jnp.concatenate([b_high, b_low], axis=0).astype(BF16)
        g = 2 * (i % 2) + (i // 2) * core + (1 - i // 2) * (1 - core)
        part = pl.ds(pl.multiple_of(g * SPAN, SPAN), SPAN)
        for n in range(4):
            columns = slice(256 * n, 256 * n + 256)
            out = mm(both, x_s[i, :, columns], NN)
            sg_s[part, :, columns] = (out[0:128] + out[128:256]).astype(BF16).reshape(SPAN, 4, 256)
            out = mm(b_both, x_s[i, 128:256, columns], NN)
            og_s[part, columns] = (out[0:SPAN] + out[SPAN : 2 * SPAN]).astype(BF16)
        return carry


    @pl.when(role < 7)
    def _():
        pl.semaphore_wait(all_in, 1)

    give(0, 0, dw1, got1, 0)
    give(0, 1, dw1, got1, 1)
    lax.fori_loop(0, 2, grads, 0)
    for a in range(2):
        dw2[a] = take(0, a, got1)
        give(1, a, dw2, got2, 1 - a)
    lax.fori_loop(2, 4, grads, 0)
    sums = [take(1, 0, got2), take(1, 1, got2)]
    per_proj = 1.0 / (4.0 * 64 * 128 * D) ** 0.5
    per_gain = 1.0 / (4.0 * 64 * 128) ** 0.5
    for q in range(8):
        a, b = q // 4, q % 4
        columns = slice(128 * q, 128 * q + 128)
        total = sums[a][6 * b : 6 * b + 6]
        pg_out[:, columns] = gain_s[:, columns] * total * per_proj
        gg_out[:, columns] = jnp.sum(total * proj_s[:, columns], axis=0, keepdims=True) * per_gain
    arrived(stat, st_send)
    arrived(got1.at[:, pl.ds(0, 7)], dw_send.at[0])
    arrived(got2.at[:, pl.ds(0, 7)], dw_send.at[1])


def store(*refs):
    copies = [pltpu.make_async_copy(refs[n], refs[4 + n], refs[8].at[n]) for n in range(4)]
    for copy in copies:
        copy.start()
    for copy in copies:
        copy.wait()


def shards(streams, layer_out, cotangent, input_cot, gain, projection, static_mix, tanh_scale):
    anywhere = pl.BlockSpec(memory_space=pl.ANY)
    vmem = pl.BlockSpec(memory_space=pltpu.VMEM)
    sg, og, pg, gg = pl.pallas_call(
        body,
        out_shape=(
            pltpu.VMEM(streams.shape, BF16),
            pltpu.VMEM(layer_out.shape, BF16),
            pltpu.VMEM((6, 1024), F32),
            pltpu.VMEM((1, 1024), F32),
        ),
        in_specs=[anywhere] * 8,
        out_specs=(vmem,) * 4,
        scratch_shapes=[
            pltpu.VMEM((GROUPS, SPAN, 4, 1024), BF16),
            pltpu.VMEM((GROUPS, SPAN, 4, 1024), BF16),
            pltpu.VMEM((GROUPS, SPAN, 1024), BF16),
            pltpu.VMEM((GROUPS, ROWS, 1024), BF16),
            pltpu.VMEM((1, 1024), F32),
            pltpu.VMEM((6, 1024), F32),
            pltpu.SMEM((4, 6), F32),
            pltpu.SMEM((3,), F32),
            pltpu.VMEM((8, 1024), F32),
            pltpu.VMEM((GROUPS, 13, 128), F32),
            pltpu.VMEM((2, 13, 128), F32),
            pltpu.VMEM((4 * GROUPS, 13, 128), F32),
            pltpu.VMEM((GROUPS, 24, 128), F32),
            pltpu.VMEM((2, 24, 128), F32),
            pltpu.VMEM((2, 24, 128), F32),
            pltpu.VMEM((2, 8, 24, 128), F32),
            pltpu.VMEM((2, 8, 24, 128), F32),
            pltpu.SemaphoreType.DMA((2,)),
            pltpu.SemaphoreType.DMA((4,)),
            pltpu.SemaphoreType.DMA((2,)),
            pltpu.SemaphoreType.DMA,
            pltpu.SemaphoreType.DMA((2,)),
            pltpu.SemaphoreType.DMA((2,)),
            pltpu.SemaphoreType.DMA((2, 2)),
            pltpu.SemaphoreType.REGULAR,
            pltpu.SemaphoreType.REGULAR,
            pltpu.SemaphoreType.REGULAR,
        ],
        compiler_params=pltpu.CompilerParams(collective_id=0, has_side_effects=True),
    )(streams, layer_out, cotangent, input_cot, gain.reshape(1, 1024), projection, static_mix, tanh_scale)
    made = (sg, og, pg, gg)
    sg, og, pg, gg = pl.pallas_call(
        store,
        out_shape=tuple(jax.ShapeDtypeStruct(a.shape, a.dtype) for a in made),
        in_specs=[vmem] * 4,
        out_specs=(anywhere,) * 4,
        scratch_shapes=[pltpu.SemaphoreType.DMA((4,))],
    )(*(pltpu.with_memory_space_constraint(a, pltpu.VMEM) for a in made))
    return sg, og, pg, gg.reshape(1024)


def solution(mesh):
    placed = (
        P("dp", None, "tensor"),
        P("dp", "tensor"),
        P("dp", None, "tensor"),
        P("dp", "tensor"),
        P("tensor"),
        P(None, "tensor"),
        P(),
        P(),
    )
    return jax.shard_map(
        shards,
        mesh=mesh,
        in_specs=placed,
        out_specs=(P("dp", None, "tensor"), P("dp", "tensor"), P(None, "tensor"), P("tensor")),
        check_vma=False,
    )
```
